256 devices in a mesh: grow: 16 (over y_lo, x, core), gcol: 16 (over z, y_hi).
Axes of the slice: x: 4, y: 4 (y_hi: 2, y_lo: 2; y = y_hi * 2 + y_lo), z: 8, core: 2. Of those that a mesh axis runs over, the one named last changes fastest.
Arguments:
- eps_static: float32 [12288, 12288], P('grow', 'gcol'), may hold values from -1.8 to 1.8
- eps_imag: float32 [12288, 12288], P('grow', 'gcol'), may hold values from -1.8 to 1.8
- frequency_grid: float32 [3], replicated, may hold values from 0.1 to 2
- band_energy: float32 [32], replicated, may hold values from -2 to 2
- pair_elements: bfloat16 [32, 64, 12288], P('grow', None, 'gcol'), may hold values from -0.0546875 to 0.0546875
Outputs:
- sigma: float32 [3, 64], P(None, 'gcol')
The draws below stay inside these ranges and needn't reach their ends.
All inputs are finite; a program needn't handle non-finite values.
Results may differ from the reference program's by a relative error of at most 0.0019.
Values may be sent and summed in bfloat16 or wider, within the bound.
No kernel may reach another device: no remote copies, remote signals or barrier semaphores. Data moves between devices by JAX's collectives and lax.ppermute only.
A program may use at most 64 MiB of HBM per device.

```python
import math
import jax
import jax.numpy as jnp
from jax import lax

NG = 12288
STATES = 64
BANDS = 32
NE = 3


def block_levels(key, extent, cuts, low, high):
    level, own = 1.0, jax.random.fold_in(key, 6)
    for position, parts in cuts:
        heights = jnp.exp(jax.random.uniform(jax.random.fold_in(own, position), (parts,), jnp.float32, low / len(cuts), high / len(cuts)))
        level = level * jnp.repeat(heights, extent[position] // parts).reshape([-1 if axis == position else 1 for axis in range(len(extent))])
    return level


def gaussian(own_key, dims, scale, limit, cuts=(), kind=jnp.bfloat16):
    entries = scale * jax.random.normal(own_key, dims, jnp.float32)
    if cuts:
        entries = entries * block_levels(own_key, dims, cuts, -0.22, 0.18)
    return jnp.clip(entries, -limit, limit).astype(kind)


def setup_inputs(seed: int = 0) -> dict:
    arg_keys = jax.random.split(jax.random.key(seed), 6)
    eps_static = gaussian(arg_keys[0], (NG, NG), 0.3, 1.8, ((0, 16), (1, 16)), jnp.float32)
    eps_imag = gaussian(arg_keys[1], (NG, NG), 0.3, 1.8, ((0, 16), (1, 16)), jnp.float32)
    frequency_grid = jnp.clip(jnp.exp(jax.random.uniform(arg_keys[2], (NE,), jnp.float32, math.log(0.1), math.log(2.0))), 0.1, 2.0)
    band_energy = jnp.clip(jax.random.uniform(arg_keys[3], (BANDS,), jnp.float32, -2.0, 2.0), -2.0, 2.0)
    pair_elements = gaussian(arg_keys[4], (BANDS, STATES, NG), NG ** -0.5, 0.0546875, ((0, 16), (2, 16)))
    return dict(eps_static=eps_static, eps_imag=eps_imag, frequency_grid=frequency_grid, band_energy=band_energy, pair_elements=pair_elements)


def pole_kernels(static_rows, imag_rows, kronecker, frequency_grid):
    static_part = static_rows - kronecker
    imag_part = imag_rows - kronecker
    spread = static_part - imag_part
    pole_square = (imag_part * imag_part + 0.25) / (spread * spread + 0.25)
    pole_freq = jnp.sqrt(pole_square)
    strength = -static_part * pole_square
    return [(strength / (pole_freq * (pole_freq + frequency_grid[point]))).astype(jnp.bfloat16) for point in range(NE)]

def reference(eps_static, eps_imag, frequency_grid, band_energy, pair_elements):
    blocks = 16
    height = NG // blocks
    rows_all = pair_elements.reshape(BANDS * STATES, NG).astype(jnp.float32)
    col_ids = lax.iota(jnp.int32, NG)
    row_ids = lax.iota(jnp.int32, height)

    def advance(block, quad):
        start = (block * height).astype(jnp.int32)
        static_rows = lax.dynamic_slice_in_dim(eps_static, start, height, 0)
        imag_rows = lax.dynamic_slice_in_dim(eps_imag, start, height, 0)
        kronecker = ((start + row_ids)[:, None] == col_ids[None, :]).astype(jnp.float32)
        kernels = pole_kernels(static_rows, imag_rows, kronecker, frequency_grid)
        left = lax.dynamic_slice_in_dim(rows_all, start, height, 1)
        terms = []
        for kernel in kernels:
            wide = lax.optimization_barrier(kernel).astype(jnp.float32)
            projected = jnp.dot(left, wide, precision=lax.Precision.HIGHEST)
            terms.append(lax.optimization_barrier(jnp.sum(projected * rows_all, axis=1)))
        return quad + jnp.stack(terms)
    quad = lax.fori_loop(0, blocks, advance, jnp.zeros((NE, BANDS * STATES), jnp.float32))
    quad = quad.reshape(NE, BANDS, STATES)
    offset = frequency_grid[:, None] - band_energy[None, :]
    weight = 1.0 / (1.0 + offset * offset)
    return jnp.einsum('em,ems->es', weight, quad)
```

```python
import itertools

import jax
import jax.numpy as jnp
from jax import lax
from jax.experimental import pallas as pl
from jax.experimental.pallas import tpu as pltpu
from jax.sharding import Mesh
from jax.sharding import PartitionSpec as P

NE = 3
GROW = ("yl", "x", "c")
GCOL = ("z", "yh")
ALL = GROW + GCOL
SIZES = (2, 4, 2, 8, 2)
LANES = 128
TILE = 256


def flat(place):
    out = 0
    for size, p in zip(SIZES, place):
        out = out * size + p
    return out


def permutation(move):
    places = itertools.product(*(range(n) for n in SIZES))
    return [(flat(p), flat(move(*p))) for p in places]


TURN = permutation(lambda yl, x, c, z, yh: (z // 4, z % 4, yh, z ^ (yl * 4 + x), c))
TURN_PEER = permutation(lambda yl, x, c, z, yh: (z // 4, z % 4, yh, z ^ (yl * 4 + x), 1 - c))


def turned(shard, order):
    return lax.ppermute(shard, ALL, order)


def shifted(shard, axis, step):
    size = lax.axis_size(axis)
    return lax.ppermute(shard, axis, [(i, (i + step) % size) for i in range(size)])


def pole_body(place, grid_points, static_ref, imag_ref, out_ref):
    height, breadth = static_ref.shape
    row = lax.broadcasted_iota(jnp.int32, (height, breadth), 0) + pl.program_id(0) * height
    col = lax.broadcasted_iota(jnp.int32, (height, breadth), 1)
    same = jnp.where(place[0] == place[1], 0, breadth)
    kronecker = (row == col + same).astype(jnp.float32)
    static_part = static_ref[...] - kronecker
    imag_part = imag_ref[...] - kronecker
    spread = static_part - imag_part
    pole_freq = jnp.sqrt((imag_part * imag_part + 0.25) / (spread * spread + 0.25))
    top = -static_part * pole_freq
    for e in range(NE):
        out_ref[e] = (top / (pole_freq + grid_points[e])).astype(jnp.bfloat16)


def pole_kernels(place, frequency_grid, eps_static, eps_imag):
    height, breadth = eps_static.shape
    step = 96
    smem = pl.BlockSpec(memory_space=pltpu.SMEM)
    block = pl.BlockSpec((step, breadth), lambda i: (i, 0))
    return pl.pallas_call(
        pole_body,
        grid=(height // step,),
        in_specs=[smem, smem, block, block],
        out_specs=pl.BlockSpec((NE, step, breadth), lambda i: (0, i, 0)),
        out_shape=jax.ShapeDtypeStruct((NE, height, breadth), jnp.bfloat16),
        cost_estimate=pl.CostEstimate(
            flops=40 * height * breadth, transcendentals=5 * height * breadth, bytes_accessed=14 * height * breadth
        ),
        name="poles",
    )(place, frequency_grid, eps_static, eps_imag)


def band_body(steps, parts, first, place, weight, *refs):
    if not first:
        acc_ref, refs = refs[0], refs[1:]
    kern_ref, own_ref, other_ref = refs[:3]
    left_refs, out_ref, right_buf, sems = refs[3 : 3 + len(parts)], refs[-3], refs[-2], refs[-1]
    yl, x, c, z, yh = (place[2 + k] for k in range(5))
    rows = own_ref.shape[1]
    states = rows // 2
    groups = []
    for k, (dz, dy) in enumerate(steps):
        source = ((z + dz) & 7) ^ (yl * 4 + x)
        core = yh ^ dy
        slot = 2 * (((source & 3) - x) & 3) + ((source >> 2) ^ yl)
        groups.append(source * 2 + core)

        @pl.when(core == c)
        def _():
            pltpu.make_async_copy(own_ref.at[slot], right_buf.at[k], sems.at[k]).start()

        @pl.when(core != c)
        def _():
            pltpu.make_async_copy(other_ref.at[slot], right_buf.at[k], sems.at[k]).start()

    left = jnp.concatenate([r[...] for r in left_refs], axis=0)
    count = len(steps)
    breadth = kern_ref.shape[2]
    for k in range(count):
        pltpu.make_async_copy(own_ref.at[0], right_buf.at[k], sems.at[k]).wait()
    for e in range(NE):
        total = jnp.zeros((count * rows, LANES), jnp.float32)
        for t in range(breadth // TILE):
            projected = jnp.dot(
                left, kern_ref[e, :, t * TILE : (t + 1) * TILE], preferred_element_type=jnp.float32
            )
            right = right_buf[:, :, t * TILE : (t + 1) * TILE].reshape(count * rows, TILE)
            product = projected * right.astype(jnp.float32)
            total = total + (product[:, :LANES] + product[:, LANES:])
        out = jnp.zeros((states, LANES), jnp.float32) if first else acc_ref[e]
        for k in range(count):
            for b in range(2):
                start = k * rows + b * states
                out = out + weight[e, groups[k] * 2 + b] * total[start : start + states]
        out_ref[e] = out


def band_terms(steps, place, weight, acc, kernels, own, other, lefts):
    rows, height = own.shape[1:]
    states = rows // 2
    count = len(steps)
    parts = [p.shape[0] for p in lefts]
    smem = pl.BlockSpec(memory_space=pltpu.SMEM)
    vmem = pl.BlockSpec(memory_space=pltpu.VMEM)
    hbm = pl.BlockSpec(memory_space=pl.ANY)
    first = acc is None
    flops = 2 * NE * count * rows * height * kernels.shape[2]
    return pl.pallas_call(
        lambda *refs: band_body(steps, parts, first, *refs),
        in_specs=[smem, smem] + ([] if first else [vmem]) + [vmem, hbm, hbm] + [vmem] * len(lefts),
        out_specs=vmem,
        out_shape=jax.ShapeDtypeStruct((NE, states, LANES), jnp.float32),
        scratch_shapes=[
            pltpu.VMEM((count, rows, kernels.shape[2]), jnp.bfloat16),
            pltpu.SemaphoreType.DMA((count,)),
        ],
        cost_estimate=pl.CostEstimate(flops=flops, transcendentals=0, bytes_accessed=4 << 20),
        name="bands",
    )(place, weight, *([] if first else [acc]), kernels, own, other, *lefts)


def summed_on_arrival(shard, axis):
    devices = lax.axis_size(axis)
    parts = jnp.moveaxis(shard.reshape(NE, devices, -1), 1, 0)
    return jnp.sum(lax.all_to_all(parts, axis, 0, 0, tiled=True), axis=0)


def of_everyone(shard, axis):
    copies = jnp.broadcast_to(shard, (lax.axis_size(axis), *shard.shape))
    return jnp.sum(lax.all_to_all(copies, axis, 0, 0, tiled=True), axis=0)


def shards(eps_static, eps_imag, frequency_grid, band_energy, pair_elements):
    place = jnp.stack([lax.axis_index(GROW), lax.axis_index(GCOL)] + [lax.axis_index(a) for a in ALL])
    bands, states, breadth = pair_elements.shape
    rows = bands * states
    shard = pair_elements.reshape(rows, breadth)
    offset_energy = frequency_grid[:, None] - band_energy[None, :]
    weight = 1.0 / (1.0 + offset_energy * offset_energy)

    mine, peer = turned(shard, TURN), turned(shard, TURN_PEER)
    both = jnp.concatenate([mine, peer])
    kernels = pole_kernels(place, frequency_grid, eps_static, eps_imag)

    pair = jnp.concatenate([shard, shifted(shard, "yl", 1)])
    before, after = shifted(pair, "x", 1), shifted(pair, "x", -1)
    far = [shifted(before[:rows], "x", 1), shifted(after[rows:], "x", -1)]
    own = jnp.concatenate([pair, after, *far, before]).reshape(8, rows, breadth)
    other = shifted(own, "c", 1)

    acc = band_terms([(0, 0), (0, 1)], place, weight, None, kernels, own, other, [both])
    up, down = both, both
    for k in (1, 2, 3):
        up, down = shifted(up, "z", 1), shifted(down, "z", -1)
        steps = [(-k, 0), (-k, 1), (k, 0), (k, 1)]
        acc = band_terms(steps, place, weight, acc, kernels, own, other, [up, down])
    last = [shifted(up[:rows], "z", 1), shifted(down[rows:], "z", -1)]
    acc = band_terms([(4, 0), (4, 1)], place, weight, acc, kernels, own, other, last)
    partial_sigma = jnp.sum(acc, axis=2)
    return of_everyone(summed_on_arrival(partial_sigma, GCOL), GROW)


def solution(mesh):
    finer = Mesh(mesh.devices.reshape(SIZES), ALL)
    in_specs = (P(GROW, GCOL), P(GROW, GCOL), P(), P(), P(GROW, None, GCOL))
    return jax.shard_map(
        shards, mesh=finer, in_specs=in_specs, out_specs=P(None, GCOL), check_vma=False
    )
```
